32 devices in a mesh: node: 8 (over y, x, core), row: 4 (over z).
Axes of the slice: x: 2, y: 2, z: 4, core: 2. Of those that a mesh axis runs over, the one named last changes fastest.
Arguments:
- samples: bfloat16 [8, 4096, 384], P('node', 'row'), parts along dimension 0, may hold values from -6 to 6
- column_order: int32 [8, 384], P('node'), parts along dimension 0, may hold values from 0 to 383, each once within a row
- skeleton: int32 [8, 256], P('node'), parts along dimension 0, may hold values from 0 to 4095, as said below
Outputs:
- q_factor: float32 [8, 4096, 384], P('node', 'row'), parts along dimension 0
- interp: bfloat16 [8, 4096, 256], P('node', 'row'), parts along dimension 0
The draws below stay inside these ranges and needn't reach their ends.
There are 8 independent parts, one for each index of `node`. The reference program is written for one: setup_inputs(seed, part) draws one part's arguments, and reference() takes and returns one part's arrays. A program takes and returns all parts, laid end to end along the dimension named above; each array names one. Nothing has to cross between parts.
Inputs may be any that keep to these rules, and one draw needn't show every extreme that they name: `skeleton`: each row names 256 distinct sample rows in ascending order. `column_order`: each row is a permutation.
All inputs are finite; a program needn't handle non-finite values.
Results may differ from the reference program's by a relative error of at most 0.001.
Values sent between devices are 32-bit elements; how exact they have to be, the bound alone decides.
No kernel may reach another device: no remote copies, remote signals or barrier semaphores. Data moves between devices by JAX's collectives and lax.ppermute only.
A program may use at most 64 MiB of HBM per device.

```python
import jax
import jax.numpy as jnp
from jax import lax

C = 384
K = 256
ROWS_DEV = 1024
FRONTS = 1
ROWS = 4096
N_ROW = 4


def draw_skeleton(key, part):
    keys = jax.random.split(jax.random.fold_in(key, 7), FRONTS)

    def pick(single):
        return jnp.sort(jax.random.permutation(single, ROWS_DEV * N_ROW)[:K]).astype(jnp.int32)
    return jax.vmap(pick)(keys)


def shard_levels(own_key, extent, shards, least, top_value):
    loudness, own = 1.0, jax.random.fold_in(own_key, 6)
    for dim, shards_of in shards:
        heights = jnp.exp(jax.random.uniform(jax.random.fold_in(own, dim), (shards_of,), jnp.float32, least / len(shards), top_value / len(shards)))
        loudness = loudness * jnp.repeat(heights, extent[dim] // shards_of).reshape([-1 if axis == dim else 1 for axis in range(len(extent))])
    return loudness


def centred(rng, extent, deviation, reach, cuts=(), held_as=jnp.bfloat16):
    factor_of = shard_levels(rng, extent, cuts, -0.22, 0.18) if cuts else 1.0
    entries = jax.random.normal(rng, extent, jnp.float32) * deviation * factor_of
    return jnp.minimum(jnp.maximum(entries, -reach), reach).astype(held_as)


def setup_inputs(seed: int = 0, part: int = 0) -> dict:
    arg_keys = jax.random.split(jax.random.key(seed), 4)
    part_keys = jax.random.split(jax.random.fold_in(arg_keys[3], part), 4)
    samples = centred(part_keys[0], (FRONTS, ROWS, C), 1.0, 6.0, ((1, 4),))
    column_order = jax.vmap(lambda own: jax.random.permutation(own, C))(jax.random.split(part_keys[1], FRONTS)).reshape((FRONTS, C)).astype(jnp.int32)
    skeleton = draw_skeleton(jax.random.fold_in(jax.random.fold_in(arg_keys[3], part), 71), part)
    return {"samples": samples, "column_order": column_order, "skeleton": skeleton}


def one_front(block, order, skel):
    permuted = block[:, order].astype(jnp.float32)
    gram = jnp.dot(permuted.T, permuted, precision=lax.Precision.HIGHEST) / ROWS
    lower = jnp.linalg.cholesky(gram)
    q_factor = jax.scipy.linalg.solve_triangular(lower, permuted.T, lower=True).T
    qskel = q_factor[skel.astype(jnp.int32)]
    small = jnp.dot(qskel, qskel.T, precision=lax.Precision.HIGHEST)
    lower_small = jnp.linalg.cholesky(small)
    cross = jnp.dot(q_factor, qskel.T, precision=lax.Precision.HIGHEST)
    inner = jax.scipy.linalg.solve_triangular(lower_small, cross.T, lower=True)
    interp = jax.scipy.linalg.solve_triangular(lower_small, inner, lower=True, trans='T').T
    return (q_factor, interp.astype(jnp.bfloat16))

def reference(samples, column_order, skeleton):
    q_factor, interp = jax.vmap(one_front)(samples, column_order, skeleton)
    return (q_factor, interp)
```

```python
import jax
import jax.numpy as jnp
from jax import lax
from jax.experimental import pallas as pl
from jax.experimental.pallas import tpu as pltpu
from jax.sharding import PartitionSpec as P

F32 = jnp.float32
BF16 = jnp.bfloat16
LANES = 128
STRIP = 32
GROUPS = STRIP // 8


def split(x):
    high = x.astype(BF16)
    low = (x - high.astype(F32)).astype(BF16)
    return high, low


def dot(a, b, dims):
    return lax.dot_general(a, b, (dims, ((), ())), preferred_element_type=F32)


NN = ((1,), (0,))
NT = ((1,), (1,))
TN = ((0,), (0,))


def exact_left(a, b, dims):
    high, low = split(b)
    return dot(a, high, dims) + dot(a, low, dims)


def product(a, b, dims):
    ah, al = split(a)
    bh, bl = split(b)
    return dot(ah, bh, dims) + (dot(ah, bl, dims) + dot(al, bh, dims))


def row_of(x, s):
    return jnp.broadcast_to(x[s : s + 1, :], (8, LANES))


def factor_strip(tiles, lane):
    diag = tiles[0]
    cols = [
        [jnp.broadcast_to(diag[g][:, lane + j : lane + j + 1], (8, LANES)) if g >= j // 8 else None for g in range(GROUPS)]
        for j in range(STRIP)
    ]
    tiles = [list(t) for t in tiles]
    sub = lax.broadcasted_iota(jnp.int32, (8, LANES), 0)
    for k in range(STRIP):
        g0, s = divmod(k, 8)
        inv = lax.rsqrt(row_of(cols[k][g0], s))
        low = [cols[k][g] * inv if g >= g0 else None for g in range(GROUPS)]
        for j in range(k + 1, STRIP):
            factor = row_of(low[j // 8], j % 8)
            for g in range(j // 8, GROUPS):
                cols[j][g] = cols[j][g] - low[g] * factor
        below = jnp.where(sub > s, low[g0], 0.0)
        for t in tiles:
            row = row_of(t[g0], s) * inv
            t[g0] = jnp.where(sub == s, row, t[g0] - below * row)
            for g in range(g0 + 1, GROUPS):
                t[g] = t[g] - low[g] * row
    return tiles


def factor(a_ref, t_ref, n):
    tiles_n = n // LANES
    row_ids = lax.broadcasted_iota(jnp.int32, (LANES, LANES), 0)
    col_ids = lax.broadcasted_iota(jnp.int32, (LANES, LANES), 1)
    for i in range(tiles_n):
        for j in range(tiles_n):
            t_ref[LANES * i : LANES * (i + 1), LANES * j : LANES * (j + 1)] = (
                jnp.where(row_ids == col_ids, 1.0, 0.0) if i == j else jnp.zeros((LANES, LANES), F32)
            )

    def spots(panel):
        return [(a_ref, t) for t in range(panel, tiles_n)] + [(t_ref, t) for t in range(panel + 1)]

    def update(rows, panel, first, last):
        size = rows.stop - rows.start
        left = a_ref[first:last, rows]
        lh, ll = split(left)
        left3 = jnp.concatenate([lh, lh, ll], axis=0)
        where = spots(panel)
        right = [split(ref[first:last, LANES * t : LANES * (t + 1)]) for ref, t in where]
        right3 = jnp.concatenate(
            [jnp.concatenate([h, l, h], axis=0) for h, l in right], axis=1
        )
        out = dot(left3, right3, TN)
        for i, (ref, t) in enumerate(where):
            at = slice(LANES * t, LANES * (t + 1))
            ref[rows, at] = ref[rows, at] - out[:, LANES * i : LANES * (i + 1)]

    per = LANES // STRIP
    for panel in range(tiles_n):
        base = LANES * panel
        for strip in range(per):
            r0 = base + STRIP * strip
            where = spots(panel)
            tiles = [
                [ref[r0 + 8 * g : r0 + 8 * g + 8, LANES * t : LANES * (t + 1)] for g in range(GROUPS)] for ref, t in where
            ]
            tiles = factor_strip(tiles, STRIP * strip)
            for (ref, t), tile in zip(where, tiles):
                for g in range(GROUPS):
                    ref[r0 + 8 * g : r0 + 8 * g + 8, LANES * t : LANES * (t + 1)] = tile[g]
            if strip + 1 < per:
                update(slice(r0 + STRIP, base + LANES), panel, r0, r0 + STRIP)
        if panel + 1 < tiles_n:
            update(slice(base + LANES, n), panel, base, base + LANES)


def upper_blocks(count):
    return [(i, j) for i in range(count) for j in range(i, count)]


def block(i):
    return slice(LANES * i, LANES * (i + 1))


def gram_kernel(order_ref, x_ref, p_ref, g_ref):
    c = x_ref.shape[1]
    source = lax.broadcasted_iota(jnp.int32, (c, c), 0)
    select = jnp.where(source == order_ref[0:1, :], 1.0, 0.0).astype(BF16)
    p = dot(x_ref[...], select, NN).astype(BF16)
    p_ref[...] = p
    for at, (i, j) in enumerate(upper_blocks(c // LANES)):
        g_ref[at] = dot(p[:, block(i)], p[:, block(j)], TN)


def pick_kernel(offset_ref, skel_ref, p_ref, y_ref):
    rows = p_ref.shape[0]
    k = skel_ref.shape[0]
    here = lax.broadcasted_iota(jnp.int32, (k, rows), 1) + offset_ref[0]
    select = jnp.where(here == skel_ref[:, 0:1], 1.0, 0.0).astype(BF16)
    y_ref[...] = dot(select, p_ref[...], NN)


def make_factor_kernel(total_rows):
    def factor_kernel(g_ref, h_ref, t_ref, a_ref):
        c = t_ref.shape[0]
        for at, (i, j) in enumerate(upper_blocks(c // LANES)):
            a_ref[block(i), block(j)] = (g_ref[at] + h_ref[at]) * (1.0 / total_rows)
        factor(a_ref, t_ref, c)

    return factor_kernel


def finish_kernel(p_ref, t_ref, y_ref, z_ref, q_ref, w_ref, a_ref, s_ref):
    k = y_ref.shape[0]
    t = t_ref[...]
    y = (y_ref[...] + z_ref[...]).astype(BF16)
    p = p_ref[...]
    qskel = exact_left(y, t, NT)
    a_ref[...] = product(qskel, qskel, NT)
    q = exact_left(p, t, NT)
    q_ref[...] = q
    cross = product(q, qskel, NT)
    factor(a_ref, s_ref, k)
    s = s_ref[...]
    inverse = product(s, s, TN)
    w_ref[...] = product(cross, inverse, NN).astype(BF16)


def vmem(shape, dtype):
    return pltpu.VMEM(shape, dtype)


PARAMS = pltpu.CompilerParams(vmem_limit_bytes=48 * 1024 * 1024)


def rounds(size):
    out, width = [], 2
    while width <= size:
        out.append([(i, i - i % width + width - 1 - i % width) for i in range(size)])
        width *= 2
    return out


def swap(x, pairs):
    return lax.ppermute(x, "row", pairs)


def on_device(samples, column_order, skeleton):
    fronts, rows, c = samples.shape
    k = skeleton.shape[1]
    size = lax.axis_size("row")
    total_rows = rows * size
    offset = (lax.axis_index("row") * rows).astype(jnp.int32).reshape(1)
    q_all, w_all = [], []
    for f in range(fronts):
        count = len(upper_blocks(c // LANES))
        p, gram = pl.pallas_call(
            gram_kernel,
            out_shape=(jax.ShapeDtypeStruct((rows, c), BF16), jax.ShapeDtypeStruct((count, LANES, LANES), F32)),
            compiler_params=PARAMS,
            name="gram",
        )(jnp.broadcast_to(column_order[f][None, :], (8, c)), samples[f])
        y = pl.pallas_call(
            pick_kernel,
            in_specs=[pl.BlockSpec(memory_space=pltpu.SMEM), pl.BlockSpec(), pl.BlockSpec()],
            out_shape=jax.ShapeDtypeStruct((k, c), F32),
            compiler_params=PARAMS,
            name="pick",
        )(offset, jnp.broadcast_to(skeleton[f][:, None], (k, LANES)), p)
        steps = rounds(size)
        for at, pairs in enumerate(steps):
            gram_in = swap(gram, pairs)
            if at + 1 < len(steps):
                gram = gram + gram_in
        for at, pairs in enumerate(steps):
            y_in = swap(y, pairs)
            if at + 1 < len(steps):
                y = y + y_in
        t = pl.pallas_call(
            make_factor_kernel(total_rows),
            out_shape=jax.ShapeDtypeStruct((c, c), F32),
            scratch_shapes=[vmem((c, c), F32)],
            compiler_params=PARAMS,
            name="factor",
        )(gram, gram_in)
        q, w = pl.pallas_call(
            finish_kernel,
            out_shape=(jax.ShapeDtypeStruct((rows, c), F32), jax.ShapeDtypeStruct((rows, k), BF16)),
            scratch_shapes=[vmem((k, k), F32), vmem((k, k), F32)],
            compiler_params=PARAMS,
            name="finish",
        )(p, t, y, y_in)
        q_all.append(q)
        w_all.append(w)
    return jnp.stack(q_all), jnp.stack(w_all)


def solution(mesh):
    placed = (P("node", "row", None), P("node", None), P("node", None))
    return jax.shard_map(
        on_device,
        mesh=mesh,
        in_specs=placed,
        out_specs=(P("node", "row", None), P("node", "row", None)),
        check_vma=False,
    )
```

```python
import jax
import jax.numpy as jnp
from jax import lax
from jax.experimental import pallas as pl
from jax.experimental.pallas import tpu as pltpu
from jax.sharding import PartitionSpec as P


F32 = jnp.float32
BF16 = jnp.bfloat16
LANES = 128
STRIP = 32
GROUPS = STRIP // 8


def split(x):
    high = x.astype(BF16)
    low = (x - high.astype(F32)).astype(BF16)
    return high, low


def dot(a, b, dims):
    return lax.dot_general(a, b, (dims, ((), ())), preferred_element_type=F32)


NN = ((1,), (0,))
NT = ((1,), (1,))
TN = ((0,), (0,))


def exact_left(a, b, dims):
    high, low = split(b)
    return dot(a, high, dims) + dot(a, low, dims)


def product(a, b, dims):
    ah, al = split(a)
    bh, bl = split(b)
    return dot(ah, bh, dims) + (dot(ah, bl, dims) + dot(al, bh, dims))


def row_of(x, s):
    return jnp.broadcast_to(x[s : s + 1, :], (8, LANES))


def factor_strip(tiles, lane):
    diag = tiles[0]
    cols = [
        [jnp.broadcast_to(diag[g][:, lane + j : lane + j + 1], (8, LANES)) if g >= j // 8 else None for g in range(GROUPS)]
        for j in range(STRIP)
    ]
    tiles = [list(t) for t in tiles]
    sub = lax.broadcasted_iota(jnp.int32, (8, LANES), 0)
    for k in range(STRIP):
        g0, s = divmod(k, 8)
        inv = lax.rsqrt(row_of(cols[k][g0], s))
        low = [cols[k][g] * inv if g >= g0 else None for g in range(GROUPS)]
        for j in range(k + 1, STRIP):
            factor = row_of(low[j // 8], j % 8)
            for g in range(j // 8, GROUPS):
                cols[j][g] = cols[j][g] - low[g] * factor
        below = jnp.where(sub > s, low[g0], 0.0)
        for t in tiles:
            row = row_of(t[g0], s) * inv
            t[g0] = jnp.where(sub == s, row, t[g0] - below * row)
            for g in range(g0 + 1, GROUPS):
                t[g] = t[g] - low[g] * row
    return tiles


def block(i):
    return slice(LANES * i, LANES * (i + 1))


def set_identity(ref):
    row_ids = lax.broadcasted_iota(jnp.int32, (LANES, LANES), 0)
    col_ids = lax.broadcasted_iota(jnp.int32, (LANES, LANES), 1)
    last = ref.shape[1] // LANES - 1
    for j in range(last):
        ref[:, block(j)] = jnp.zeros((LANES, LANES), F32)
    ref[:, block(last)] = jnp.where(row_ids == col_ids, 1.0, 0.0)


def stack_left(x):
    high, low = split(x)
    return [high, high, low]


def stack_right(x):
    high, low = split(x)
    return [high, low, high]


def take_out(ref, rows, t, lefts, rights):
    left = jnp.concatenate([part for x in lefts for part in x], axis=0)
    right = jnp.concatenate([part for x in rights for part in stack_right(x)], axis=0)
    ref[rows, block(t)] = ref[rows, block(t)] - dot(left, right, TN)


def factor_panel(u_ref, t_ref):
    targets = [(u_ref, t) for t in range(u_ref.shape[1] // LANES)]
    targets += [(t_ref, t) for t in range(t_ref.shape[1] // LANES)]
    for r0 in range(0, LANES, STRIP):
        tiles = [[ref[r0 + 8 * g : r0 + 8 * g + 8, block(t)] for g in range(GROUPS)] for ref, t in targets]
        tiles = factor_strip(tiles, r0)
        for (ref, t), tile in zip(targets, tiles):
            for g in range(GROUPS):
                ref[r0 + 8 * g : r0 + 8 * g + 8, block(t)] = tile[g]
        if r0 + STRIP < LANES:
            rows = slice(r0 + STRIP, LANES)
            whole = [jnp.concatenate(tile, axis=0) for tile in tiles]
            left = stack_left(whole[0][:, r0 + STRIP :])
            for (ref, t), right in zip(targets, whole):
                take_out(ref, rows, t, [left], [right])


def take_out_panels(u_before, t_before, u_ref, t_ref):
    panel = len(u_before)
    if not panel:
        return
    rows = slice(0, LANES)
    lefts = [stack_left(u_before[at][:, block(panel - at)]) for at in range(panel)]
    for i in range(u_ref.shape[1] // LANES):
        take_out(u_ref, rows, i, lefts, [u_before[at][:, block(panel - at + i)] for at in range(panel)])
    for i in range(panel):
        take_out(t_ref, rows, i, lefts[i:], [t_before[at][:, block(i)] for at in range(i, panel)])


def upper_blocks(first, count):
    return [(i, j) for i in range(first, count) for j in range(i, count)]


PACKED_ROWS = LANES // 2


def pack_list(count):
    return [(i, j) for i, j in upper_blocks(0, count) if i != j or i > 1]


def message_rows(count):
    return PACKED_ROWS * (1 + len(pack_list(count))) + 8


def masks():
    row_ids = lax.broadcasted_iota(jnp.int32, (LANES, LANES), 0)
    col_ids = lax.broadcasted_iota(jnp.int32, (LANES, LANES), 1)
    return row_ids, col_ids


def gram_kernel(place_ref, order_ref, x_ref, p_ref, keep_ref, send_ref):
    c = x_ref.shape[1]
    count = c // LANES
    source = lax.broadcasted_iota(jnp.int32, (c, c), 0)
    select = jnp.where(source == order_ref[0:1, :], 1.0, 0.0).astype(BF16)
    p = dot(x_ref[...], select, NN).astype(BF16)
    p_ref[...] = p
    even = place_ref[1] == 0
    row_ids, col_ids = masks()

    def put(at, g):
        top, low = g[:PACKED_ROWS], g[PACKED_ROWS:]
        keep_ref[PACKED_ROWS * at : PACKED_ROWS * (at + 1)] = jnp.where(even, top, low)
        send_ref[PACKED_ROWS * at : PACKED_ROWS * (at + 1)] = jnp.where(even, low, top)

    d0 = dot(p[:, block(0)], p[:, block(0)], TN)
    d1 = dot(p[:, block(1)], p[:, block(1)], TN)
    put(0, jnp.where(row_ids >= col_ids, d0, d1))
    diagonal = jnp.sum(jnp.where(row_ids == col_ids, d1, 0.0), axis=0, keepdims=True)
    diagonal = jnp.broadcast_to(diagonal, (8, LANES))
    for ref in (keep_ref, send_ref):
        ref[ref.shape[0] - 8 :] = diagonal
    for at, (i, j) in enumerate(pack_list(count)):
        put(at + 1, dot(p[:, block(i)], p[:, block(j)], TN))


def unpack(even, mine_ref, other_ref, count, scale):
    def take(at):
        return join(
            even,
            mine_ref[PACKED_ROWS * at : PACKED_ROWS * (at + 1)],
            other_ref[PACKED_ROWS * at : PACKED_ROWS * (at + 1)],
        ) * scale

    row_ids, col_ids = masks()
    shared = take(0)
    turned = shared.T
    diagonal = mine_ref[mine_ref.shape[0] - 8 :][0:1] * scale
    out = {
        (0, 0): jnp.where(row_ids >= col_ids, shared, turned),
        (1, 1): jnp.where(row_ids < col_ids, shared, jnp.where(row_ids > col_ids, turned, diagonal)),
    }
    for at, spot in enumerate(pack_list(count)):
        out[spot] = take(at + 1)
    return out


def pick_kernel(place_ref, skel_ref, p_ref, keep_ref, send_ref):
    rows = p_ref.shape[0]
    k = skel_ref.shape[1]
    here = lax.broadcasted_iota(jnp.int32, (rows, k), 0) + place_ref[0]
    select = jnp.where(here == skel_ref[0:1, :], 1.0, 0.0).astype(BF16)
    y = dot(select, p_ref[...], TN)
    even = place_ref[1] == 0
    keep_ref[...] = jnp.where(even, y[: k // 2], y[k // 2 :])
    send_ref[...] = jnp.where(even, y[k // 2 :], y[: k // 2])


def join(even, mine, other):
    return jnp.concatenate([jnp.where(even, mine, other), jnp.where(even, other, mine)], axis=-2)


def make_panels_kernel(first, last, count, total_rows):
    def panels_kernel(place_ref, mine_ref, other_ref, *refs):
        us, ts = list(refs[:first]), list(refs[first : 2 * first])
        us += refs[2 * first : first + last]
        ts += refs[first + last :]
        gram = unpack(place_ref[1] == 0, mine_ref, other_ref, count, 1.0 / total_rows)
        for panel in range(first, last):
            for j in range(panel, count):
                us[panel][:, block(j - panel)] = gram[panel, j]
            set_identity(ts[panel])
            take_out_panels(us[:panel], ts[:panel], us[panel], ts[panel])
            factor_panel(us[panel], ts[panel])

    return panels_kernel


def finish_kernel(place_ref, p_ref, mine_ref, other_ref, *refs):
    t_parts = refs[:-5]
    q_ref, w_ref, tt_ref, a_ref, s_ref = refs[-5:]
    even = place_ref[1] == 0
    k = a_ref.shape[0]
    for i, part in enumerate(t_parts):
        tt_ref[block(i), : part.shape[1]] = part[...]
        if i + 1 < len(t_parts):
            tt_ref[block(i), part.shape[1] :] = jnp.zeros((LANES, tt_ref.shape[1] - part.shape[1]), F32)
    t = tt_ref[...]
    y = join(even, mine_ref[...], other_ref[...]).astype(BF16)
    p = p_ref[...]
    qskel = exact_left(y, t, NT)
    a_ref[...] = product(qskel, qskel, NT)
    q = exact_left(p, t, NT)
    q_ref[...] = q
    cross = product(q, qskel, NT)
    panels = k // LANES
    us = [a_ref.at[block(i), LANES * i :] for i in range(panels)]
    ts = [s_ref.at[block(i), : LANES * (i + 1)] for i in range(panels)]
    for i in range(panels):
        set_identity(ts[i])
        if i + 1 < panels:
            s_ref[block(i), LANES * (i + 1) :] = jnp.zeros((LANES, k - LANES * (i + 1)), F32)
        take_out_panels(us[:i], ts[:i], us[i], ts[i])
        factor_panel(us[i], ts[i])
    s = s_ref[...]
    inverse = product(s, s, TN)
    w_ref[...] = product(cross, inverse, NN).astype(BF16)


def vmem(shape, dtype):
    return pltpu.VMEM(shape, dtype)


PARAMS = pltpu.CompilerParams(vmem_limit_bytes=48 * 1024 * 1024)


def call(kernel, out_shape, place, *args, scratch=()):
    return pl.pallas_call(
        kernel,
        in_specs=[pl.BlockSpec(memory_space=pltpu.SMEM)] + [pl.BlockSpec()] * len(args),
        out_shape=out_shape,
        scratch_shapes=scratch,
        compiler_params=PARAMS,
    )(place, *args)


def shape(*dims, dtype=F32):
    return jax.ShapeDtypeStruct(dims, dtype)


def swap(x, pairs):
    return lax.ppermute(x, "row", pairs)


def neighbours(size):
    return [(i, i ^ 1) for i in range(size)]


def mirrored(size, width):
    return [(i, i ^ (width - 1)) for i in range(size)]


def share(keep, send, size):
    got = swap(send, neighbours(size))
    mine = keep + got
    width = 4
    while width <= size:
        got = swap(mine, mirrored(size, width))
        mine = mine + got
        width *= 2
    other = swap(mine, neighbours(size))
    return mine, other


def compute(samples, column_order, skeleton):
    fronts, rows, c = samples.shape
    k = skeleton.shape[1]
    size = lax.axis_size("row")
    total_rows = rows * size
    index = lax.axis_index("row")
    place = jnp.stack([index * rows, (index ^ (index >> 1)) & 1]).astype(jnp.int32)
    count = c // LANES
    q_all, w_all = [], []
    for f in range(fronts):
        p, keep, sent = call(
            gram_kernel,
            (shape(rows, c, dtype=BF16),) + (shape(message_rows(count), LANES),) * 2,
            place,
            column_order[f][None, :],
            samples[f],
        )
        keep_y, sent_y = call(pick_kernel, (shape(k // 2, c),) * 2, place, skeleton[f][None, :], p)
        mine, other = share(keep, sent, size)
        mine_y, other_y = share(keep_y, sent_y, size)
        us, ts = [], []
        cut = count - 1
        for first, last in ((0, cut), (cut, count)):
            out = call(
                make_panels_kernel(first, last, count, total_rows),
                tuple(shape(LANES, c - LANES * i) for i in range(first, last))
                + tuple(shape(LANES, LANES * (i + 1)) for i in range(first, last)),
                place,
                mine,
                other,
                *us,
                *ts,
            )
            us += out[: last - first]
            ts += out[last - first :]
        q, w = call(
            finish_kernel,
            (shape(rows, c), shape(rows, k, dtype=BF16)),
            place,
            p,
            mine_y,
            other_y,
            *ts,
            scratch=[vmem((c, c), F32), vmem((k, k), F32), vmem((k, k), F32)],
        )
        q_all.append(q)
        w_all.append(w)
    return jnp.stack(q_all), jnp.stack(w_all)


def solution(mesh):
    placed = (P("node", "row", None), P("node", None), P("node", None))
    return jax.shard_map(
        compute,
        mesh=mesh,
        in_specs=placed,
        out_specs=(P("node", "row", None), P("node", "row", None)),
        check_vma=False,
    )
```

```python
import jax
import jax.numpy as jnp
from jax import lax
from jax.experimental import pallas as pl
from jax.experimental.pallas import tpu as pltpu
from jax.sharding import PartitionSpec as P


F32 = jnp.float32
BF16 = jnp.bfloat16
LANES = 128
STRIP = 32
GROUPS = STRIP // 8


def split(x):
    high = x.astype(BF16)
    low = (x - high.astype(F32)).astype(BF16)
    return high, low


def dot(a, b, dims):
    return lax.dot_general(a, b, (dims, ((), ())), preferred_element_type=F32)


NN = ((1,), (0,))
NT = ((1,), (1,))
TN = ((0,), (0,))


def exact_left(a, b, dims):
    high, low = split(b)
    return dot(a, high, dims) + dot(a, low, dims)


def product(a, b, dims):
    ah, al = split(a)
    bh, bl = split(b)
    return dot(ah, bh, dims) + (dot(ah, bl, dims) + dot(al, bh, dims))


def row_of(x, s):
    return jnp.broadcast_to(x[s : s + 1, :], (8, LANES))


def spread(tile, lane, first, count):
    return [
        [
            jnp.broadcast_to(tile[g][:, lane + first + j : lane + first + j + 1], (8, LANES)) if g >= first // 8 else None
            for g in range(GROUPS)
        ]
        for j in range(count)
    ]


def eliminate(tile, sub, steps, first):
    tile = list(tile)
    for k, (inv, low) in enumerate(steps, first):
        g0, s = divmod(k, 8)
        row = row_of(tile[g0], s) * inv
        below = jnp.where(sub > s, low[g0], 0.0)
        tile[g0] = jnp.where(sub == s, row, tile[g0] - below * row)
        for g in range(g0 + 1, GROUPS):
            tile[g] = tile[g] - low[g] * row
    return tile


def factor_strip(diag, lane):
    sub = lax.broadcasted_iota(jnp.int32, (8, LANES), 0)
    now = spread(diag, lane, 0, 8)
    steps = []
    for first in range(0, STRIP, 8):
        after = spread(diag, lane, first + 8, 8) if first + 8 < STRIP else []
        done = []
        for k in range(8):
            g0 = first // 8
            inv = lax.rsqrt(row_of(now[k][g0], k))
            low = [now[k][g] * inv if g >= g0 else None for g in range(GROUPS)]
            for j in range(k + 1, 8):
                factor = row_of(low[g0], j)
                for g in range(g0, GROUPS):
                    now[j][g] = now[j][g] - low[g] * factor
            for j in range(len(after)):
                factor = row_of(low[g0 + 1], j)
                for g in range(g0 + 1, GROUPS):
                    after[j][g] = after[j][g] - low[g] * factor
            done.append((inv, low))
        diag = eliminate(diag, sub, done, first)
        steps += done
        now = after
    return steps, diag, sub


def block(i):
    return slice(LANES * i, LANES * (i + 1))


def set_identity(ref):
    row_ids = lax.broadcasted_iota(jnp.int32, (LANES, LANES), 0)
    col_ids = lax.broadcasted_iota(jnp.int32, (LANES, LANES), 1)
    last = ref.shape[1] // LANES - 1
    for j in range(last):
        ref[:, block(j)] = jnp.zeros((LANES, LANES), F32)
    ref[:, block(last)] = jnp.where(row_ids == col_ids, 1.0, 0.0)


def stack_left(x):
    high, low = split(x)
    return jnp.concatenate([high, high, low], axis=0).T


def stack_right(x):
    high, low = split(x)
    return [high, low, high]


def take_out(ref, rows, t, lefts, rights):
    left = lefts[0] if len(lefts) == 1 else jnp.concatenate(lefts, axis=1)
    right = jnp.concatenate([part for x in rights for part in stack_right(x)], axis=0)
    ref[rows, block(t)] = ref[rows, block(t)] - dot(left, right, NN)


def factor_panel(u_ref, t_ref, beside=None):
    targets = [(u_ref, t) for t in range(u_ref.shape[1] // LANES)]
    targets += [(t_ref, t) for t in range(t_ref.shape[1] // LANES)]
    for r0 in range(0, LANES, STRIP):
        last = r0 + STRIP == LANES
        rows = slice(r0 + STRIP, LANES)
        steps = left = sub = None
        if beside:
            beside(r0 // STRIP)
        for ref, t in targets:
            tile = [ref[r0 + 8 * g : r0 + 8 * g + 8, block(t)] for g in range(GROUPS)]
            if steps is None:
                steps, tile, sub = factor_strip(tile, r0)
            else:
                tile = eliminate(tile, sub, steps, 0)
            whole = jnp.concatenate(tile, axis=0)
            ref[r0 : r0 + STRIP, block(t)] = whole
            if not last:
                if left is None:
                    left = stack_left(whole)[r0 + STRIP :]
                take_out(ref, rows, t, [left], [whole])


def take_out_panels(u_before, t_before, u_ref, t_ref):
    panel = len(u_before)
    if not panel:
        return
    rows = slice(0, LANES)
    lefts = [stack_left(u_before[at][:, block(panel - at)]) for at in range(panel)]
    for i in range(u_ref.shape[1] // LANES):
        take_out(u_ref, rows, i, lefts, [u_before[at][:, block(panel - at + i)] for at in range(panel)])
    for i in range(panel):
        take_out(t_ref, rows, i, lefts[i:], [t_before[at][:, block(i)] for at in range(i, panel)])


def upper_blocks(first, count):
    return [(i, j) for i in range(first, count) for j in range(i, count)]


PACKED_ROWS = LANES // 2


def pack_list(count):
    return [(i, j) for i, j in upper_blocks(0, count) if i != j or i > 1]


def message_rows(count):
    return PACKED_ROWS * (1 + len(pack_list(count))) + 8


def masks():
    row_ids = lax.broadcasted_iota(jnp.int32, (LANES, LANES), 0)
    col_ids = lax.broadcasted_iota(jnp.int32, (LANES, LANES), 1)
    return row_ids, col_ids


def gram_kernel(place_ref, order_ref, x_ref, p_ref, keep_ref, send_ref):
    c = x_ref.shape[1]
    count = c // LANES
    source = lax.broadcasted_iota(jnp.int32, (c, c), 0)
    select = jnp.where(source == order_ref[0:1, :], 1.0, 0.0).astype(BF16)
    p = dot(x_ref[...], select, NN).astype(BF16)
    p_ref[...] = p
    even = place_ref[1] == 0
    row_ids, col_ids = masks()

    def put(at, g):
        top, low = g[:PACKED_ROWS], g[PACKED_ROWS:]
        keep_ref[PACKED_ROWS * at : PACKED_ROWS * (at + 1)] = jnp.where(even, top, low)
        send_ref[PACKED_ROWS * at : PACKED_ROWS * (at + 1)] = jnp.where(even, low, top)

    d0 = dot(p[:, block(0)], p[:, block(0)], TN)
    d1 = dot(p[:, block(1)], p[:, block(1)], TN)
    put(0, jnp.where(row_ids >= col_ids, d0, d1))
    diagonal = jnp.sum(jnp.where(row_ids == col_ids, d1, 0.0), axis=0, keepdims=True)
    diagonal = jnp.broadcast_to(diagonal, (8, LANES))
    for ref in (keep_ref, send_ref):
        ref[ref.shape[0] - 8 :] = diagonal
    for at, (i, j) in enumerate(pack_list(count)):
        put(at + 1, dot(p[:, block(i)], p[:, block(j)], TN))


def unpack(even, mine_ref, other_ref, count, scale):
    def take(at):
        return join(
            even,
            mine_ref[PACKED_ROWS * at : PACKED_ROWS * (at + 1)],
            other_ref[PACKED_ROWS * at : PACKED_ROWS * (at + 1)],
        ) * scale

    row_ids, col_ids = masks()
    shared = take(0)
    turned = shared.T
    diagonal = mine_ref[mine_ref.shape[0] - 8 :][0:1] * scale
    out = {
        (0, 0): jnp.where(row_ids >= col_ids, shared, turned),
        (1, 1): jnp.where(row_ids < col_ids, shared, jnp.where(row_ids > col_ids, turned, diagonal)),
    }
    for at, spot in enumerate(pack_list(count)):
        out[spot] = take(at + 1)
    return out


def pick_kernel(place_ref, skel_ref, p_ref, keep_ref, send_ref):
    rows = p_ref.shape[0]
    k = skel_ref.shape[1]
    here = lax.broadcasted_iota(jnp.int32, (rows, k), 0) + place_ref[0]
    select = jnp.where(here == skel_ref[0:1, :], 1.0, 0.0).astype(BF16)
    y = dot(select, p_ref[...], TN)
    even = place_ref[1] == 0
    keep_ref[...] = jnp.where(even, y[: k // 2], y[k // 2 :])
    send_ref[...] = jnp.where(even, y[k // 2 :], y[: k // 2])


def join(even, mine, other):
    return jnp.concatenate([jnp.where(even, mine, other), jnp.where(even, other, mine)], axis=-2)


def make_panels_kernel(first, last, count, total_rows):
    def panels_kernel(place_ref, mine_ref, other_ref, *refs):
        us, ts = list(refs[:first]), list(refs[first : 2 * first])
        us += refs[2 * first : first + last]
        ts += refs[first + last :]
        gram = unpack(place_ref[1] == 0, mine_ref, other_ref, count, 1.0 / total_rows)
        for panel in range(first, last):
            for j in range(panel, count):
                us[panel][:, block(j - panel)] = gram[panel, j]
            set_identity(ts[panel])
            take_out_panels(us[:panel], ts[:panel], us[panel], ts[panel])
            factor_panel(us[panel], ts[panel])

    return panels_kernel


def finish_kernel(place_ref, p_ref, mine_ref, other_ref, *refs):
    t_parts = refs[:-9]
    q_out, w_out, tt_ref, a_ref, s_ref, q_ref, cross_ref, w_ref, sems = refs[-9:]
    even = place_ref[1] == 0
    k = a_ref.shape[0]
    rows = p_ref.shape[0]
    for i, part in enumerate(t_parts):
        tt_ref[block(i), : part.shape[1]] = part[...]
        if i + 1 < len(t_parts):
            tt_ref[block(i), part.shape[1] :] = jnp.zeros((LANES, tt_ref.shape[1] - part.shape[1]), F32)
    t = tt_ref[...]
    y = join(even, mine_ref[...], other_ref[...]).astype(BF16)
    qskel = exact_left(y, t, NT)
    a_ref[...] = product(qskel, qskel, NT)
    panels = k // LANES
    per = LANES // STRIP
    pieces = panels * per
    piece = rows // pieces
    copies = []

    def write(src, dst, i, sem):
        at = pl.ds(piece * i, piece)
        copies.append(pltpu.make_async_copy(src.at[at], dst.at[at], sem))
        copies[-1].start()

    def beside(i):
        if i:
            write(q_ref, q_out, i - 1, sems.at[0, i - 1])
        at = slice(piece * i, piece * (i + 1))
        q = exact_left(p_ref[at], t, NT)
        q_ref[at] = q
        cross_ref[at] = product(q, qskel, NT)

    us = [a_ref.at[block(i), LANES * i :] for i in range(panels)]
    ts = [s_ref.at[block(i), : LANES * (i + 1)] for i in range(panels)]
    for i in range(panels):
        set_identity(ts[i])
        if i + 1 < panels:
            s_ref[block(i), LANES * (i + 1) :] = jnp.zeros((LANES, k - LANES * (i + 1)), F32)
        take_out_panels(us[:i], ts[:i], us[i], ts[i])
        factor_panel(us[i], ts[i], lambda strip, i=i: beside(per * i + strip))
    write(q_ref, q_out, pieces - 1, sems.at[0, pieces - 1])
    s = s_ref[...]
    inverse = product(s, s, TN)
    for i in range(pieces):
        at = slice(piece * i, piece * (i + 1))
        w_ref[at] = product(cross_ref[at], inverse, NN).astype(BF16)
        if i:
            write(w_ref, w_out, i - 1, sems.at[1, i - 1])
    write(w_ref, w_out, pieces - 1, sems.at[1, pieces - 1])
    for copy in copies:
        copy.wait()


def vmem(shape, dtype):
    return pltpu.VMEM(shape, dtype)


PARAMS = pltpu.CompilerParams(vmem_limit_bytes=48 * 1024 * 1024)


def call(kernel, out_shape, place, *args, scratch=(), **kwargs):
    return pl.pallas_call(
        kernel,
        in_specs=[pl.BlockSpec(memory_space=pltpu.SMEM)] + [pl.BlockSpec()] * len(args),
        out_shape=out_shape,
        scratch_shapes=scratch,
        compiler_params=PARAMS,
        **kwargs,
    )(place, *args)


def shape(*dims, dtype=F32):
    return jax.ShapeDtypeStruct(dims, dtype)


def swap(x, pairs):
    return lax.ppermute(x, "row", pairs)


def neighbours(size):
    return [(i, i ^ 1) for i in range(size)]


def mirrored(size, width):
    return [(i, i ^ (width - 1)) for i in range(size)]


def share(keep, send, size):
    got = swap(send, neighbours(size))
    mine = keep + got
    width = 4
    while width <= size:
        got = swap(mine, mirrored(size, width))
        mine = mine + got
        width *= 2
    other = swap(mine, neighbours(size))
    return mine, other


def compute(samples, column_order, skeleton):
    fronts, rows, c = samples.shape
    k = skeleton.shape[1]
    size = lax.axis_size("row")
    total_rows = rows * size
    index = lax.axis_index("row")
    place = jnp.stack([index * rows, (index ^ (index >> 1)) & 1]).astype(jnp.int32)
    count = c // LANES
    q_all, w_all = [], []
    for f in range(fronts):
        p, keep, sent = call(
            gram_kernel,
            (shape(rows, c, dtype=BF16),) + (shape(message_rows(count), LANES),) * 2,
            place,
            column_order[f][None, :],
            samples[f],
        )
        keep_y, sent_y = call(pick_kernel, (shape(k // 2, c),) * 2, place, skeleton[f][None, :], p)
        mine, other = share(keep, sent, size)
        mine_y, other_y = share(keep_y, sent_y, size)
        us, ts = [], []
        cut = count - 1
        for first, last in ((0, cut), (cut, count)):
            out = call(
                make_panels_kernel(first, last, count, total_rows),
                tuple(shape(LANES, c - LANES * i) for i in range(first, last))
                + tuple(shape(LANES, LANES * (i + 1)) for i in range(first, last)),
                place,
                mine,
                other,
                *us,
                *ts,
            )
            us += out[: last - first]
            ts += out[last - first :]
        q, w = call(
            finish_kernel,
            (shape(rows, c), shape(rows, k, dtype=BF16)),
            place,
            p,
            mine_y,
            other_y,
            *ts,
            scratch=[
                vmem((c, c), F32),
                vmem((k, k), F32),
                vmem((k, k), F32),
                vmem((rows, c), F32),
                vmem((rows, k), F32),
                vmem((rows, k), BF16),
                pltpu.SemaphoreType.DMA((2, k // STRIP)),
            ],
            out_specs=(pl.BlockSpec(memory_space=pl.ANY),) * 2,
        )
        q_all.append(q)
        w_all.append(w)
    return jnp.stack(q_all), jnp.stack(w_all)


def solution(mesh):
    placed = (P("node", "row", None), P("node", None), P("node", None))
    return jax.shard_map(
        compute,
        mesh=mesh,
        in_specs=placed,
        out_specs=(P("node", "row", None), P("node", "row", None)),
        check_vma=False,
    )
```

```python
import jax
import jax.numpy as jnp
from jax import lax
from jax.experimental import pallas as pl
from jax.experimental.pallas import tpu as pltpu
from jax.sharding import PartitionSpec as P


F32 = jnp.float32
BF16 = jnp.bfloat16
LANES = 128
STRIP = 32
GROUPS = STRIP // 8


def split(x):
    high = x.astype(BF16)
    low = (x - high.astype(F32)).astype(BF16)
    return high, low


def dot(a, b, dims):
    return lax.dot_general(a, b, (dims, ((), ())), preferred_element_type=F32)


NN = ((1,), (0,))
NT = ((1,), (1,))
TN = ((0,), (0,))


def exact_left(a, b, dims):
    high, low = split(b)
    return dot(a, high, dims) + dot(a, low, dims)


def product(a, b, dims):
    ah, al = split(a)
    bh, bl = split(b)
    return dot(ah, bh, dims) + (dot(ah, bl, dims) + dot(al, bh, dims))


def row_of(x, s):
    return jnp.broadcast_to(x[s : s + 1, :], (8, LANES))


def spread(tile, lane, first, count):
    return [
        [
            jnp.broadcast_to(tile[g][:, lane + first + j : lane + first + j + 1], (8, LANES)) if g >= first // 8 else None
            for g in range(GROUPS)
        ]
        for j in range(count)
    ]


def eliminate(tile, sub, steps, first):
    tile = list(tile)
    for k, (inv, low) in enumerate(steps, first):
        g0, s = divmod(k, 8)
        row = row_of(tile[g0], s) * inv
        below = jnp.where(sub > s, low[g0], 0.0)
        tile[g0] = jnp.where(sub == s, row, tile[g0] - below * row)
        for g in range(g0 + 1, GROUPS):
            tile[g] = tile[g] - low[g] * row
    return tile


def factor_strip(diag, lane):
    sub = lax.broadcasted_iota(jnp.int32, (8, LANES), 0)
    now = spread(diag, lane, 0, 8)
    steps = []
    for first in range(0, STRIP, 8):
        after = spread(diag, lane, first + 8, 8) if first + 8 < STRIP else []
        done = []
        for k in range(8):
            g0 = first // 8
            inv = lax.rsqrt(row_of(now[k][g0], k))
            low = [now[k][g] * inv if g >= g0 else None for g in range(GROUPS)]
            for j in range(k + 1, 8):
                factor = row_of(low[g0], j)
                for g in range(g0, GROUPS):
                    now[j][g] = now[j][g] - low[g] * factor
            for j in range(len(after)):
                factor = row_of(low[g0 + 1], j)
                for g in range(g0 + 1, GROUPS):
                    after[j][g] = after[j][g] - low[g] * factor
            done.append((inv, low))
        diag = eliminate(diag, sub, done, first)
        steps += done
        now = after
    return steps, diag, sub


def block(i):
    return slice(LANES * i, LANES * (i + 1))


def set_identity(ref):
    row_ids = lax.broadcasted_iota(jnp.int32, (LANES, LANES), 0)
    col_ids = lax.broadcasted_iota(jnp.int32, (LANES, LANES), 1)
    last = ref.shape[1] // LANES - 1
    for j in range(last):
        ref[:, block(j)] = jnp.zeros((LANES, LANES), F32)
    ref[:, block(last)] = jnp.where(row_ids == col_ids, 1.0, 0.0)


def stack_left(x):
    high, low = split(x)
    return jnp.concatenate([high, high, low], axis=0).T


def stack_right(x):
    high, low = split(x)
    return [high, low, high]


def take_out(ref, rows, t, lefts, rights):
    left = lefts[0] if len(lefts) == 1 else jnp.concatenate(lefts, axis=1)
    right = jnp.concatenate([part for x in rights for part in stack_right(x)], axis=0)
    ref[rows, block(t)] = ref[rows, block(t)] - dot(left, right, NN)


def factor_panel(u_ref, t_ref, beside=None):
    targets = [(u_ref, t) for t in range(u_ref.shape[1] // LANES)]
    targets += [(t_ref, t) for t in range(t_ref.shape[1] // LANES)]
    for r0 in range(0, LANES, STRIP):
        last = r0 + STRIP == LANES
        rows = slice(r0 + STRIP, LANES)
        steps = left = sub = None
        if beside:
            beside(r0 // STRIP)
        for ref, t in targets:
            tile = [ref[r0 + 8 * g : r0 + 8 * g + 8, block(t)] for g in range(GROUPS)]
            if steps is None:
                steps, tile, sub = factor_strip(tile, r0)
            else:
                tile = eliminate(tile, sub, steps, 0)
            whole = jnp.concatenate(tile, axis=0)
            ref[r0 : r0 + STRIP, block(t)] = whole
            if not last:
                if left is None:
                    left = stack_left(whole)[r0 + STRIP :]
                take_out(ref, rows, t, [left], [whole])


def take_out_panels(u_before, t_before, u_ref, t_ref):
    panel = len(u_before)
    if not panel:
        return
    rows = slice(0, LANES)
    lefts = [stack_left(u_before[at][:, block(panel - at)]) for at in range(panel)]
    for i in range(u_ref.shape[1] // LANES):
        take_out(u_ref, rows, i, lefts, [u_before[at][:, block(panel - at + i)] for at in range(panel)])
    for i in range(panel):
        take_out(t_ref, rows, i, lefts[i:], [t_before[at][:, block(i)] for at in range(i, panel)])


def upper_blocks(first, count):
    return [(i, j) for i in range(first, count) for j in range(i, count)]


PACKED_ROWS = LANES // 2


FOLDED_ROWS = 3 * LANES // 8


def pack_list(count):
    out, at = [], PACKED_ROWS
    for i, j in upper_blocks(0, count):
        if i != j or i > 1:
            out.append((i, j, at, FOLDED_ROWS if i == j else PACKED_ROWS))
            at += out[-1][-1]
    return out


def message_rows(count):
    return pack_list(count)[-1][2] + pack_list(count)[-1][3] + 8


def fold(g):
    half, quarter = LANES // 2, LANES // 4
    right = lax.broadcasted_iota(jnp.int32, (quarter, LANES), 1) >= half
    low = jnp.where(right, g[half : half + quarter], pltpu.roll(g[half + quarter :], half, 1))
    return jnp.concatenate([g[:half], low], axis=0)


def unfold(g):
    half = LANES // 2
    low = g[half:]
    return jnp.concatenate([g[:half], low, pltpu.roll(low, half, 1)], axis=0)


def masks():
    row_ids = lax.broadcasted_iota(jnp.int32, (LANES, LANES), 0)
    col_ids = lax.broadcasted_iota(jnp.int32, (LANES, LANES), 1)
    return row_ids, col_ids


def gram_kernel(place_ref, order_ref, x_ref, p_ref, keep_ref, send_ref):
    c = x_ref.shape[1]
    count = c // LANES
    source = lax.broadcasted_iota(jnp.int32, (c, c), 0)
    select = jnp.where(source == order_ref[0:1, :], 1.0, 0.0).astype(BF16)
    p = dot(x_ref[...], select, NN).astype(BF16)
    p_ref[...] = p
    even = place_ref[1] == 0
    row_ids, col_ids = masks()

    def put(at, size, g):
        top, low = g[:size], g[size:]
        keep_ref[at : at + size] = jnp.where(even, top, low)
        send_ref[at : at + size] = jnp.where(even, low, top)

    d0 = dot(p[:, block(0)], p[:, block(0)], TN)
    d1 = dot(p[:, block(1)], p[:, block(1)], TN)
    put(0, PACKED_ROWS, jnp.where(row_ids >= col_ids, d0, d1))
    diagonal = jnp.sum(jnp.where(row_ids == col_ids, d1, 0.0), axis=0, keepdims=True)
    diagonal = jnp.broadcast_to(diagonal, (8, LANES))
    for ref in (keep_ref, send_ref):
        ref[ref.shape[0] - 8 :] = diagonal
    for i, j, at, size in pack_list(count):
        g = dot(p[:, block(i)], p[:, block(j)], TN)
        put(at, size, fold(g) if i == j else g)


def unpack(even, mine_ref, other_ref, count, scale):
    def take(at, size):
        return join(even, mine_ref[at : at + size], other_ref[at : at + size]) * scale

    row_ids, col_ids = masks()
    shared = take(0, PACKED_ROWS)
    turned = shared.T
    diagonal = mine_ref[mine_ref.shape[0] - 8 :][0:1] * scale
    out = {
        (0, 0): jnp.where(row_ids >= col_ids, shared, turned),
        (1, 1): jnp.where(row_ids < col_ids, shared, jnp.where(row_ids > col_ids, turned, diagonal)),
    }
    for i, j, at, size in pack_list(count):
        out[i, j] = unfold(take(at, size)) if i == j else take(at, size)
    return out


def pick_kernel(place_ref, skel_ref, p_ref, keep_ref, send_ref):
    rows = p_ref.shape[0]
    k = skel_ref.shape[1]
    here = lax.broadcasted_iota(jnp.int32, (rows, k), 0) + place_ref[0]
    select = jnp.where(here == skel_ref[0:1, :], 1.0, 0.0).astype(BF16)
    y = dot(select, p_ref[...], TN)
    even = place_ref[1] == 0
    keep_ref[...] = jnp.where(even, y[: k // 2], y[k // 2 :])
    send_ref[...] = jnp.where(even, y[k // 2 :], y[: k // 2])


def join(even, mine, other):
    return jnp.concatenate([jnp.where(even, mine, other), jnp.where(even, other, mine)], axis=-2)


def make_panels_kernel(first, last, count, total_rows):
    def panels_kernel(place_ref, mine_ref, other_ref, *refs):
        us, ts = list(refs[:first]), list(refs[first : 2 * first])
        us += refs[2 * first : first + last]
        ts += refs[first + last :]
        gram = unpack(place_ref[1] == 0, mine_ref, other_ref, count, 1.0 / total_rows)
        for panel in range(first, last):
            for j in range(panel, count):
                us[panel][:, block(j - panel)] = gram[panel, j]
            set_identity(ts[panel])
            take_out_panels(us[:panel], ts[:panel], us[panel], ts[panel])
            factor_panel(us[panel], ts[panel])

    return panels_kernel


def finish_kernel(place_ref, p_ref, mine_ref, other_ref, *refs):
    t_parts = refs[:-9]
    q_out, w_out, tt_ref, a_ref, s_ref, q_ref, cross_ref, w_ref, sems = refs[-9:]
    even = place_ref[1] == 0
    k = a_ref.shape[0]
    rows = p_ref.shape[0]
    for i, part in enumerate(t_parts):
        tt_ref[block(i), : part.shape[1]] = part[...]
        if i + 1 < len(t_parts):
            tt_ref[block(i), part.shape[1] :] = jnp.zeros((LANES, tt_ref.shape[1] - part.shape[1]), F32)
    t = tt_ref[...]
    y = join(even, mine_ref[...], other_ref[...]).astype(BF16)
    qskel = exact_left(y, t, NT)
    a_ref[...] = product(qskel, qskel, NT)
    panels = k // LANES
    per = LANES // STRIP
    pieces = panels * per
    piece = rows // pieces
    copies = []

    def write(src, dst, i, sem):
        at = pl.ds(piece * i, piece)
        copies.append(pltpu.make_async_copy(src.at[at], dst.at[at], sem))
        copies[-1].start()

    def beside(i):
        if i:
            write(q_ref, q_out, i - 1, sems.at[0, i - 1])
        at = slice(piece * i, piece * (i + 1))
        q = exact_left(p_ref[at], t, NT)
        q_ref[at] = q
        cross_ref[at] = product(q, qskel, NT)

    us = [a_ref.at[block(i), LANES * i :] for i in range(panels)]
    ts = [s_ref.at[block(i), : LANES * (i + 1)] for i in range(panels)]
    for i in range(panels):
        set_identity(ts[i])
        if i + 1 < panels:
            s_ref[block(i), LANES * (i + 1) :] = jnp.zeros((LANES, k - LANES * (i + 1)), F32)
        take_out_panels(us[:i], ts[:i], us[i], ts[i])
        factor_panel(us[i], ts[i], lambda strip, i=i: beside(per * i + strip))
    write(q_ref, q_out, pieces - 1, sems.at[0, pieces - 1])
    s = s_ref[...]
    inverse = product(s, s, TN)
    for i in range(pieces):
        at = slice(piece * i, piece * (i + 1))
        w_ref[at] = product(cross_ref[at], inverse, NN).astype(BF16)
        if i:
            write(w_ref, w_out, i - 1, sems.at[1, i - 1])
    write(w_ref, w_out, pieces - 1, sems.at[1, pieces - 1])
    for copy in copies:
        copy.wait()


def vmem(shape, dtype):
    return pltpu.VMEM(shape, dtype)


PARAMS = pltpu.CompilerParams(vmem_limit_bytes=48 * 1024 * 1024)


def call(kernel, out_shape, place, *args, scratch=(), **kwargs):
    return pl.pallas_call(
        kernel,
        in_specs=[pl.BlockSpec(memory_space=pltpu.SMEM)] + [pl.BlockSpec()] * len(args),
        out_shape=out_shape,
        scratch_shapes=scratch,
        compiler_params=PARAMS,
        **kwargs,
    )(place, *args)


def shape(*dims, dtype=F32):
    return jax.ShapeDtypeStruct(dims, dtype)


def swap(x, pairs):
    return lax.ppermute(x, "row", pairs)


def neighbours(size):
    return [(i, i ^ 1) for i in range(size)]


def mirrored(size, width):
    return [(i, i ^ (width - 1)) for i in range(size)]


def share(keep, send, size):
    got = swap(send, neighbours(size))
    mine = keep + got
    width = 4
    while width <= size:
        got = swap(mine, mirrored(size, width))
        mine = mine + got
        width *= 2
    other = swap(mine, neighbours(size))
    return mine, other


def compute(samples, column_order, skeleton):
    fronts, rows, c = samples.shape
    k = skeleton.shape[1]
    size = lax.axis_size("row")
    total_rows = rows * size
    index = lax.axis_index("row")
    place = jnp.stack([index * rows, (index ^ (index >> 1)) & 1]).astype(jnp.int32)
    count = c // LANES
    q_all, w_all = [], []
    for f in range(fronts):
        p, keep, sent = call(
            gram_kernel,
            (shape(rows, c, dtype=BF16),) + (shape(message_rows(count), LANES),) * 2,
            place,
            column_order[f][None, :],
            samples[f],
        )
        keep_y, sent_y = call(pick_kernel, (shape(k // 2, c),) * 2, place, skeleton[f][None, :], p)
        mine, other = share(keep, sent, size)
        mine_y, other_y = share(keep_y, sent_y, size)
        us, ts = [], []
        cut = count - 1
        for first, last in ((0, cut), (cut, count)):
            out = call(
                make_panels_kernel(first, last, count, total_rows),
                tuple(shape(LANES, c - LANES * i) for i in range(first, last))
                + tuple(shape(LANES, LANES * (i + 1)) for i in range(first, last)),
                place,
                mine,
                other,
                *us,
                *ts,
            )
            us += out[: last - first]
            ts += out[last - first :]
        q, w = call(
            finish_kernel,
            (shape(rows, c), shape(rows, k, dtype=BF16)),
            place,
            p,
            mine_y,
            other_y,
            *ts,
            scratch=[
                vmem((c, c), F32),
                vmem((k, k), F32),
                vmem((k, k), F32),
                vmem((rows, c), F32),
                vmem((rows, k), F32),
                vmem((rows, k), BF16),
                pltpu.SemaphoreType.DMA((2, k // STRIP)),
            ],
            out_specs=(pl.BlockSpec(memory_space=pl.ANY),) * 2,
        )
        q_all.append(q)
        w_all.append(w)
    return jnp.stack(q_all), jnp.stack(w_all)


def solution(mesh):
    placed = (P("node", "row", None), P("node", None), P("node", None))
    return jax.shard_map(
        compute,
        mesh=mesh,
        in_specs=placed,
        out_specs=(P("node", "row", None), P("node", "row", None)),
        check_vma=False,
    )
```
